128 devices in a mesh: dp: 32 (over z, y, x_hi), expert: 2 (over core), tensor: 2 (over x_lo).
Axes of the slice: x: 4 (x_hi: 2, x_lo: 2; x = x_hi * 2 + x_lo), y: 4, z: 4, core: 2. Of those that a mesh axis runs over, the one named last changes fastest.
Arguments:
- dense_act: bfloat16 [2, 128, 512, 3584], P(None, 'dp', 'expert', 'tensor'), may hold values from -6 to 6
- dense_cot: bfloat16 [2, 128, 512, 3584], P(None, 'dp', ('expert', 'tensor')), may hold values from -6 to 6
- dense_proj_in: bfloat16 [2, 3584, 128], P(None, 'tensor'), may hold values from -0.09375 to 0.09375
- dense_proj_out: bfloat16 [2, 3584, 128], replicated, may hold values from -0.09375 to 0.09375
- expert_act: bfloat16 [128, 8, 64, 2560], P('dp', 'expert', None, 'tensor'), may hold values from -6 to 6
- expert_cot: bfloat16 [128, 8, 64, 3584], P('dp', 'expert', 'tensor'), may hold values from -6 to 6
- expert_proj_in: bfloat16 [2560, 128], P('tensor'), may hold values from -0.125 to 0.125
- expert_proj_out: bfloat16 [3584, 128], replicated, may hold values from -0.09375 to 0.09375
- dense_valid: float32 [2, 128, 128], replicated, may hold values from -0.0012207031 to 0.0012207031
- expert_valid: float32 [8, 128, 128], P('expert'), may hold values from -0.0012207031 to 0.0012207031
- domain_ids: int32 [128], P('dp'), may hold values from 0 to 63
- prior_mix: float32 [64], replicated, may hold values from 0.002 to 0.05
Outputs:
- log_mixture_weights: float32 [64], P('dp')
The draws below stay inside these ranges and needn't reach their ends.
All inputs are finite; a program needn't handle non-finite values.
Results may differ from the reference program's by a relative error of at most 0.0003.
Values sent between devices are 32-bit elements; how exact they have to be, the bound alone decides.
A program may use at most 128 MiB of HBM per device.

```python
import math
import jax
import jax.numpy as jnp
from jax import lax

D = 3584
FFE = 2560
R = 128
LAYERS = 2
DOMAINS = 64
TOK_MB = 512
CAP = 64
MICRO = 128
EXPERTS = 8


def plant(array, own_key, low, high):
    place = [jax.random.randint(jax.random.fold_in(own_key, axis), (), 0, length) for axis, length in enumerate(array.shape)]
    main_axis = array.shape.index(max(array.shape))
    neighbour = place[:main_axis] + [(place[main_axis] + 1) % array.shape[main_axis]] + place[main_axis + 1:]
    return array.at[tuple(place)].set(low).at[tuple(neighbour)].set(high)


def steps_of(own_key, extent, cuts, smallest, high):
    def one(position, shards_of):
        heights = jax.random.uniform(jax.random.fold_in(jax.random.fold_in(own_key, 6), position), (shards_of,), jnp.float32, smallest / len(cuts), high / len(cuts))
        return jnp.repeat(jnp.exp(heights), extent[position] // shards_of).reshape((-1,) + (1,) * (len(extent) - position - 1))

    loudness = one(*cuts[0])
    for cut in cuts[1:]:
        loudness = loudness * one(*cut)
    return loudness


def gaussian(key, shape, scale, reach, split=(), kind=jnp.bfloat16):
    entries = jax.random.normal(key, shape, jnp.float32) * scale
    if len(split) > 0:
        entries = steps_of(key, shape, split, -0.22, 0.18) * entries
    return jnp.clip(entries, min=-reach, max=reach).astype(kind)


def setup_inputs(seed: int = 0) -> dict:
    key_list = jax.random.split(jax.random.key(seed), 13)
    dense_act = gaussian(key_list[0], (LAYERS, MICRO, TOK_MB, D), 1.0, 6.0, ((1, 32), (2, 2), (3, 2)))
    dense_cot = gaussian(key_list[1], (LAYERS, MICRO, TOK_MB, D), 1.0, 6.0, ((1, 32), (2, 4)))
    dense_proj_in = gaussian(key_list[2], (LAYERS, D, R), D ** -0.5, 0.09375, ((1, 2),))
    dense_proj_out = gaussian(key_list[3], (LAYERS, D, R), D ** -0.5, 0.09375)
    expert_act = gaussian(key_list[4], (MICRO, EXPERTS, CAP, FFE), 1.0, 6.0, ((0, 32), (1, 2), (3, 2)))
    expert_cot = gaussian(key_list[5], (MICRO, EXPERTS, CAP, D), 1.0, 6.0, ((0, 32), (1, 2), (2, 2)))
    expert_proj_in = gaussian(key_list[6], (FFE, R), FFE ** -0.5, 0.125, ((0, 2),))
    expert_proj_out = gaussian(key_list[7], (D, R), D ** -0.5, 0.09375)
    dense_valid = gaussian(key_list[8], (LAYERS, R, R), (R * R * (LAYERS * TOK_MB + EXPERTS * CAP)) ** -0.5, 0.0012207031, (), jnp.float32)
    expert_valid = gaussian(key_list[9], (EXPERTS, R, R), (R * R * (LAYERS * TOK_MB + EXPERTS * CAP)) ** -0.5, 0.0012207031, ((0, 2),), jnp.float32)
    domain_ids = plant(jax.random.randint(key_list[10], (MICRO,), 0, DOMAINS), jax.random.fold_in(key_list[10], 1), 0, DOMAINS - 1).astype(jnp.int32)
    prior_mix = jnp.clip(jnp.exp(jax.random.uniform(key_list[11], (DOMAINS,), jnp.float32, math.log(0.002), math.log(0.05))), 0.002, 0.05)
    return dict(dense_act=dense_act, dense_cot=dense_cot, dense_proj_in=dense_proj_in, dense_proj_out=dense_proj_out, expert_act=expert_act, expert_cot=expert_cot, expert_proj_in=expert_proj_in, expert_proj_out=expert_proj_out, dense_valid=dense_valid, expert_valid=expert_valid, domain_ids=domain_ids, prior_mix=prior_mix)


def reference(dense_act, dense_cot, dense_proj_in, dense_proj_out, expert_act, expert_cot, expert_proj_in, expert_proj_out, dense_valid, expert_valid, domain_ids, prior_mix):
    width = dense_act.shape[3]
    micro = dense_act.shape[1]
    tokens = dense_act.shape[2]
    rank = dense_proj_in.shape[2]
    score = jnp.zeros((micro,), jnp.float32)
    for layer in range(dense_act.shape[0]):
        dense_update_vector = jnp.dot(dense_act[layer].reshape(-1, width), dense_proj_in[layer], preferred_element_type=jnp.float32).reshape(micro, tokens, rank)
        dense_weight_matrix = jnp.dot(dense_cot[layer].reshape(-1, width), dense_proj_out[layer], preferred_element_type=jnp.float32).reshape(micro, tokens, rank)
        sketch = jnp.einsum('mtr,mts->mrs', dense_update_vector, dense_weight_matrix, precision=lax.Precision.HIGHEST)
        score = score + lax.optimization_barrier(jnp.sum(sketch * dense_valid[layer][None], axis=(1, 2)))
    experts = expert_act.shape[1]
    slots = expert_act.shape[2]
    expert_u = jnp.dot(expert_act.reshape(-1, expert_act.shape[3]), expert_proj_in, preferred_element_type=jnp.float32).reshape(micro, experts, slots, rank)
    expert_weight_matrix = jnp.dot(expert_cot.reshape(-1, width), expert_proj_out, preferred_element_type=jnp.float32).reshape(micro, experts, slots, rank)
    expert_sketch = jnp.einsum('mecr,mecs->mers', expert_u, expert_weight_matrix, precision=lax.Precision.HIGHEST)
    score = score + lax.optimization_barrier(jnp.sum(expert_sketch * expert_valid[None], axis=(1, 2, 3)))
    domains = prior_mix.shape[0]
    onehot = (domain_ids[:, None] == jnp.arange(domains, dtype=jnp.int32)[None, :]).astype(jnp.float32)
    domain_total = jnp.dot(score, onehot, precision=lax.Precision.HIGHEST)
    spread = jnp.sqrt(jnp.mean(domain_total * domain_total) + 1e-06)
    z_value = domain_total / spread
    mass = jnp.sum(prior_mix * jnp.exp(0.5 * z_value))
    return jnp.log(prior_mix) + 0.5 * z_value - jnp.log(mass)
```

```python
import functools

import jax
import jax.numpy as jnp
from jax import lax
from jax.experimental import pallas as pl
from jax.experimental.pallas import tpu as pltpu
from jax.sharding import PartitionSpec as P

MESH = pl.DeviceIdType.MESH
F32 = jnp.float32
EXACT = lax.Precision.HIGHEST


def fold(product):
    rows, lanes = product.shape
    return jnp.sum(product.reshape(rows // 8, 8, lanes), axis=0)


def kernel(
    sizes,
    dense_act,
    dense_cot,
    dense_proj_in,
    dense_proj_out,
    expert_act,
    expert_cot,
    expert_proj_in,
    expert_proj_out,
    dense_valid,
    expert_valid,
    domain_ids,
    prior_mix,
    out,
    da,
    dc,
    pin,
    pout,
    ea,
    ec,
    epin,
    epout,
    dval,
    evalid,
    ids,
    prior,
    send,
    recv,
    wv,
    acc,
    row,
    rows,
    load_sem,
    send_sem,
    recv_sem,
    row_send_sem,
    row_recv_sem,
):
    n_dp, n_e, n_t = sizes
    devices = n_dp * n_e * n_t
    dp, ex, te = lax.axis_index("dp"), lax.axis_index("expert"), lax.axis_index("tensor")
    me = (dp * n_e + ex) * n_t + te
    layers, micro = dense_act.shape[0], dense_act.shape[1]
    half = dense_cot.shape[2]
    experts, slots = expert_cot.shape[1], expert_cot.shape[2]
    chunks = micro + layers * micro
    partner = {"tensor": 1 - te}

    def device(lid):
        return {
            "dp": lid // (n_e * n_t),
            "expert": (lid // n_t) % n_e,
            "tensor": lid % n_t,
        }

    loads = {}

    def load(name, src, dst):
        copy = pltpu.make_async_copy(src, dst, load_sem.at[len(loads)])
        loads[name] = copy

    other = pl.multiple_of((1 - te) * half, half)
    mine = pl.multiple_of(te * half, half)
    e_other = pl.multiple_of((1 - te) * slots, slots)
    e_mine = pl.multiple_of(te * slots, slots)
    load("epin", expert_proj_in, epin)
    for m in range(micro):
        load(("eao", m), expert_act.at[m, :, pl.ds(e_other, slots), :], ea.at[0, m])
    for l in range(layers):
        load(("pin", l), dense_proj_in.at[l], pin.at[l])
        for m in range(micro):
            load(("dao", l, m), dense_act.at[l, m, pl.ds(other, half), :], da.at[0, l, m])
    n_first = len(loads)
    load("ids", domain_ids, ids)
    load("prior", prior_mix, prior)
    load("epout", expert_proj_out, epout)
    load("evalid", expert_valid, evalid)
    load("dval", dense_valid, dval)
    for m in range(micro):
        load(("eam", m), expert_act.at[m, :, pl.ds(e_mine, slots), :], ea.at[1, m])
        load(("ec", m), expert_cot.at[m], ec.at[m])
    for l in range(layers):
        load(("pout", l), dense_proj_out.at[l], pout.at[l])
        for m in range(micro):
            load(("dam", l, m), dense_act.at[l, m, pl.ds(mine, half), :], da.at[1, l, m])
            load(("dc", l, m), dense_cot.at[l, m], dc.at[l, m])
    names = list(loads)
    for name in names[:n_first]:
        loads[name].start()

    barrier = pltpu.get_barrier_semaphore()

    def greet(k, carry):
        pl.semaphore_signal(
            barrier, inc=1, device_id=device((me + k) % devices), device_id_type=MESH
        )
        return carry

    lax.fori_loop(1, devices, greet, 0)

    def exchange(i):
        return pltpu.make_async_remote_copy(
            src_ref=send.at[i],
            dst_ref=recv.at[i],
            send_sem=send_sem.at[i],
            recv_sem=recv_sem.at[i],
            device_id=partner,
            device_id_type=MESH,
        )

    def project(block, weight):
        return jnp.dot(block, weight, preferred_element_type=F32)

    loads["epin"].wait()
    for m in range(micro):
        loads["eao", m].wait()
        block = ea[0, m].reshape(experts * slots, -1)
        send[m] = project(block, epin[...])
        if m == 0:
            pl.semaphore_wait(barrier, devices - 1)
        exchange(m).start()
        if m == 0:
            for name in names[n_first:]:
                loads[name].start()
    for l in range(layers):
        loads["pin", l].wait()
        for m in range(micro):
            loads["dao", l, m].wait()
            i = micro + l * micro + m
            send[i] = project(da[0, l, m], pin[l])
            exchange(i).start()

    for name in ("epout", "evalid", "dval"):
        loads[name].wait()
    for m in range(micro):
        loads["eam", m].wait()
        loads["ec", m].wait()
        u = project(ea[1, m].reshape(experts * slots, -1), epin[...])
        w = project(ec[m].reshape(experts * slots, -1), epout[...])
        parts = [
            lax.dot_general(
                w[e * slots : (e + 1) * slots],
                evalid[e],
                (((1,), (1,)), ((), ())),
                precision=EXACT,
                preferred_element_type=F32,
            )
            for e in range(experts)
        ]
        wv_i = jnp.concatenate(parts, axis=0)
        wv[m] = wv_i
        acc[m] = fold(u * wv_i)
    for l in range(layers):
        loads["pout", l].wait()
        for m in range(micro):
            loads["dam", l, m].wait()
            loads["dc", l, m].wait()
            i = micro + l * micro + m
            u = project(da[1, l, m], pin[l])
            w = project(dc[l, m], pout[l])
            wv_i = lax.dot_general(
                w, dval[l], (((1,), (1,)), ((), ())), precision=EXACT, preferred_element_type=F32
            )
            wv[i] = wv_i
            acc[m] += fold(u * wv_i)

    loads["ids"].wait()
    loads["prior"].wait()
    for i in range(chunks):
        m = i % micro
        exchange(i).wait_recv()
        acc[m] += fold(recv[i] * wv[i])

    lane = lax.broadcasted_iota(jnp.int32, (1, 128), 1)
    mine_row = jnp.zeros((1, 128), F32)
    for m in range(micro):
        s = jnp.sum(jnp.sum(acc[m], axis=0, keepdims=True), axis=1, keepdims=True)
        mine_row += jnp.where(lane == ids[m], s, 0.0)

    row[...] = mine_row
    rows[me] = mine_row

    def tell(k, carry):
        pltpu.make_async_remote_copy(
            src_ref=row,
            dst_ref=rows.at[me],
            send_sem=row_send_sem,
            recv_sem=row_recv_sem,
            device_id=device((me + k) % devices),
            device_id_type=MESH,
        ).start()
        return carry

    lax.fori_loop(1, devices, tell, 0)
    everyone = pltpu.make_async_remote_copy(
        src_ref=rows.at[pl.ds(0, devices - 1)],
        dst_ref=rows.at[pl.ds(0, devices - 1)],
        send_sem=row_send_sem,
        recv_sem=row_recv_sem,
        device_id=partner,
        device_id_type=MESH,
    )
    everyone.wait_recv()
    total = jnp.sum(rows[...], axis=0)

    domains = prior_mix.shape[0]
    total = total[:, :domains]
    mix = prior[...].reshape(1, domains)
    spread = jnp.sqrt(jnp.sum(total * total, axis=1, keepdims=True) / domains + 1e-06)
    z = total / spread
    mass = jnp.sum(mix * jnp.exp(0.5 * z), axis=1, keepdims=True)
    result = jnp.log(mix) + 0.5 * z - jnp.log(mass)
    share = domains // n_dp
    place = lax.broadcasted_iota(jnp.int32, (1, domains), 1)
    for j in range(share):
        out[j] = jnp.sum(jnp.where(place == dp * share + j, result, 0.0))

    everyone.wait_send()
    for i in range(chunks):
        exchange(i).wait_send()


def per_device(*args):
    (
        dense_act,
        dense_cot,
        dense_proj_in,
        dense_proj_out,
        expert_act,
        expert_cot,
        expert_proj_in,
        expert_proj_out,
        dense_valid,
        expert_valid,
        domain_ids,
        prior_mix,
    ) = args
    sizes = tuple(lax.axis_size(name) for name in ("dp", "expert", "tensor"))
    devices = sizes[0] * sizes[1] * sizes[2]
    layers, micro, tokens, feat = dense_act.shape
    half, width = dense_cot.shape[2:]
    experts, caps, hidden = expert_act.shape[1:]
    slots = expert_cot.shape[2]
    rank = dense_proj_in.shape[2]
    bf = dense_act.dtype
    chunks = micro + layers * micro
    n_loads = 1 + micro + layers * (1 + micro) + 5 + 2 * micro + layers * (1 + 2 * micro)
    return pl.pallas_call(
        functools.partial(kernel, sizes),
        out_shape=jax.ShapeDtypeStruct((prior_mix.shape[0] // sizes[0],), F32),
        in_specs=[pl.BlockSpec(memory_space=pl.ANY)] * len(args),
        out_specs=pl.BlockSpec(memory_space=pltpu.SMEM),
        scratch_shapes=[
            pltpu.VMEM((2, layers, micro, half, feat), bf),
            pltpu.VMEM((layers, micro, half, width), bf),
            pltpu.VMEM((layers, feat, rank), bf),
            pltpu.VMEM((layers, width, rank), bf),
            pltpu.VMEM((2, micro, experts, slots, hidden), bf),
            pltpu.VMEM((micro, experts, slots, width), bf),
            pltpu.VMEM((hidden, rank), bf),
            pltpu.VMEM((width, rank), bf),
            pltpu.VMEM(dense_valid.shape, F32),
            pltpu.VMEM(expert_valid.shape, F32),
            pltpu.SMEM(domain_ids.shape, jnp.int32),
            pltpu.VMEM(prior_mix.shape, F32),
            pltpu.VMEM((chunks, half, rank), F32),
            pltpu.VMEM((chunks, half, rank), F32),
            pltpu.VMEM((chunks, half, rank), F32),
            pltpu.VMEM((micro, 8, rank), F32),
            pltpu.VMEM((1, 128), F32),
            pltpu.VMEM((devices, 1, 128), F32),
            pltpu.SemaphoreType.DMA((n_loads,)),
            pltpu.SemaphoreType.DMA((chunks,)),
            pltpu.SemaphoreType.DMA((chunks,)),
            pltpu.SemaphoreType.DMA,
            pltpu.SemaphoreType.DMA,
        ],
        compiler_params=pltpu.CompilerParams(
            collective_id=0, has_side_effects=True, vmem_limit_bytes=60 << 20
        ),
        name="align",
    )(*args)


def solution(mesh):
    placed = (
        P(None, "dp", "expert", "tensor"),
        P(None, "dp", ("expert", "tensor"), None),
        P(None, "tensor", None),
        P(),
        P("dp", "expert", None, "tensor"),
        P("dp", "expert", "tensor", None),
        P("tensor", None),
        P(),
        P(),
        P("expert", None, None),
        P("dp"),
        P(),
    )
    return jax.shard_map(per_device, mesh=mesh, in_specs=placed, out_specs=P("dp"), check_vma=False)
```

```python
import functools

import jax
import jax.numpy as jnp
from jax import lax
from jax.experimental import pallas as pl
from jax.experimental.pallas import tpu as pltpu
from jax.sharding import PartitionSpec as P

MESH = pl.DeviceIdType.MESH
F32 = jnp.float32
EXACT = lax.Precision.HIGHEST


def fold(product):
    rows, lanes = product.shape
    return jnp.sum(product.reshape(rows // 8, 8, lanes), axis=0)


def kernel(
    sizes,
    dense_act,
    dense_cot,
    dense_proj_in,
    dense_proj_out,
    expert_act,
    expert_cot,
    expert_proj_in,
    expert_proj_out,
    dense_valid,
    expert_valid,
    domain_ids,
    prior_mix,
    out,
    da,
    dc,
    pin,
    pout,
    ea,
    ec,
    epin,
    epout,
    dval,
    evalid,
    ids,
    prior,
    send,
    recv,
    wv,
    acc,
    row,
    rows,
    here,
    load_sem,
    send_sem,
    recv_sem,
    row_send_sem,
    row_recv_sem,
):
    n_dp, n_e, n_t = sizes
    devices = n_dp * n_e * n_t
    dp, ex, te = lax.axis_index("dp"), lax.axis_index("expert"), lax.axis_index("tensor")
    me = (dp * n_e + ex) * n_t + te
    layers, micro = dense_act.shape[0], dense_act.shape[1]
    half = dense_cot.shape[2]
    experts, slots = expert_cot.shape[1], expert_cot.shape[2]
    chunks = micro + layers * micro
    partner = {"tensor": 1 - te}

    ring = 4
    x, y, z = (dp % 2) * 2 + te, (dp // 2) % ring, dp // (2 * ring)

    def away(offset):
        dc, dx, dy, dz = offset
        cc = (ex + dc) % n_e
        xx, yy, zz = (x + dx) % ring, (y + dy) % ring, (z + dz) % ring
        return (((zz * ring + yy) * 2 + xx // n_t) * n_e + cc) * n_t + xx % n_t

    around = [(1, 0, 0, 0)]
    for axis in (1, 2, 3):
        for step in (1, ring - 1):
            around.append(tuple(step if k == axis else 0 for k in range(4)))
    lines = {
        axis: [tuple(step if k == axis else 0 for k in range(4)) for step in range(1, ring)]
        for axis in (1, 2, 3)
    }
    rounds = [around, lines[1], lines[2], around[:1]]

    def hello(semaphore, offsets):
        for offset in offsets:
            pl.semaphore_signal(
                semaphore, inc=1, device_id=away(offset), device_id_type=pl.DeviceIdType.LOGICAL
            )

    loads = {}

    def load(name, src, dst):
        copy = pltpu.make_async_copy(src, dst, load_sem.at[len(loads)])
        loads[name] = copy

    other = pl.multiple_of((1 - te) * half, half)
    mine = pl.multiple_of(te * half, half)
    e_other = pl.multiple_of((1 - te) * slots, slots)
    e_mine = pl.multiple_of(te * slots, slots)
    load("epin", expert_proj_in, epin)
    for m in range(micro):
        load(("eao", m), expert_act.at[m, :, pl.ds(e_other, slots), :], ea.at[0, m])
    for l in range(layers):
        load(("pin", l), dense_proj_in.at[l], pin.at[l])
        for m in range(micro):
            load(("dao", l, m), dense_act.at[l, m, pl.ds(other, half), :], da.at[0, l, m])
    n_first = len(loads)
    load("ids", domain_ids, ids)
    load("prior", prior_mix, prior)
    load("epout", expert_proj_out, epout)
    load("evalid", expert_valid, evalid)
    load("dval", dense_valid, dval)
    for m in range(micro):
        load(("eam", m), expert_act.at[m, :, pl.ds(e_mine, slots), :], ea.at[1, m])
        load(("ec", m), expert_cot.at[m], ec.at[m])
    for l in range(layers):
        load(("pout", l), dense_proj_out.at[l], pout.at[l])
        for m in range(micro):
            load(("dam", l, m), dense_act.at[l, m, pl.ds(mine, half), :], da.at[1, l, m])
            load(("dc", l, m), dense_cot.at[l, m], dc.at[l, m])
    names = list(loads)
    for name in names[:n_first]:
        loads[name].start()

    barrier = pltpu.get_barrier_semaphore()
    hello(barrier, around)

    def exchange(i):
        return pltpu.make_async_remote_copy(
            src_ref=send.at[i],
            dst_ref=recv.at[i],
            send_sem=send_sem.at[i],
            recv_sem=recv_sem.at[i],
            device_id=partner,
            device_id_type=MESH,
        )

    def project(block, weight):
        return jnp.dot(block, weight, preferred_element_type=F32)

    loads["epin"].wait()
    for m in range(micro):
        loads["eao", m].wait()
        block = ea[0, m].reshape(experts * slots, -1)
        send[m] = project(block, epin[...])
        if m == 0:
            pl.semaphore_wait(barrier, len(around))
            hello(here.at[0], rounds[0])
        exchange(m).start()
        if m == 0:
            for name in names[n_first:]:
                loads[name].start()
    for l in range(layers):
        loads["pin", l].wait()
        for m in range(micro):
            loads["dao", l, m].wait()
            i = micro + l * micro + m
            send[i] = project(da[0, l, m], pin[l])
            exchange(i).start()

    for name in ("epout", "evalid", "dval"):
        loads[name].wait()
    for m in range(micro):
        pl.semaphore_wait(here.at[m], len(rounds[m]))
        if m + 1 < len(rounds):
            hello(here.at[m + 1], rounds[m + 1])
        loads["eam", m].wait()
        loads["ec", m].wait()
        u = project(ea[1, m].reshape(experts * slots, -1), epin[...])
        w = project(ec[m].reshape(experts * slots, -1), epout[...])
        parts = [
            lax.dot_general(
                w[e * slots : (e + 1) * slots],
                evalid[e],
                (((1,), (1,)), ((), ())),
                precision=EXACT,
                preferred_element_type=F32,
            )
            for e in range(experts)
        ]
        wv_i = jnp.concatenate(parts, axis=0)
        wv[m] = wv_i
        acc[m] = fold(u * wv_i)
    for l in range(layers):
        loads["pout", l].wait()
        for m in range(micro):
            loads["dam", l, m].wait()
            loads["dc", l, m].wait()
            i = micro + l * micro + m
            u = project(da[1, l, m], pin[l])
            w = project(dc[l, m], pout[l])
            wv_i = lax.dot_general(
                w, dval[l], (((1,), (1,)), ((), ())), precision=EXACT, preferred_element_type=F32
            )
            wv[i] = wv_i
            acc[m] += fold(u * wv_i)

    loads["ids"].wait()
    loads["prior"].wait()
    for i in range(chunks):
        m = i % micro
        exchange(i).wait_recv()
        acc[m] += fold(recv[i] * wv[i])

    lane = lax.broadcasted_iota(jnp.int32, (1, 128), 1)
    mine_row = jnp.zeros((1, 128), F32)
    for m in range(micro):
        s = jnp.sum(jnp.sum(acc[m], axis=0, keepdims=True), axis=1, keepdims=True)
        mine_row += jnp.where(lane == ids[m], s, 0.0)

    row[...] = mine_row
    rows[me] = mine_row

    hops = lambda offset: sum(min(d, n - d) for d, n in zip(offset, (2, ring, ring, ring)))
    offsets = [
        (dc, dx, dy, dz)
        for dc in range(n_e)
        for dx in range(ring)
        for dy in range(ring)
        for dz in range(ring)
    ][1:]
    offsets.sort(key=hops, reverse=True)
    for offset in offsets:
        pltpu.make_async_remote_copy(
            src_ref=row,
            dst_ref=rows.at[me],
            send_sem=row_send_sem,
            recv_sem=row_recv_sem,
            device_id=away(offset),
            device_id_type=pl.DeviceIdType.LOGICAL,
        ).start()
    everyone = pltpu.make_async_remote_copy(
        src_ref=rows.at[pl.ds(0, devices - 1)],
        dst_ref=rows.at[pl.ds(0, devices - 1)],
        send_sem=row_send_sem,
        recv_sem=row_recv_sem,
        device_id=partner,
        device_id_type=MESH,
    )
    everyone.wait_recv()
    total = jnp.sum(rows[...], axis=0)

    domains = prior_mix.shape[0]
    total = total[:, :domains]
    mix = prior[...].reshape(1, domains)
    spread = jnp.sqrt(jnp.sum(total * total, axis=1, keepdims=True) / domains + 1e-06)
    z = total / spread
    mass = jnp.sum(mix * jnp.exp(0.5 * z), axis=1, keepdims=True)
    result = jnp.log(mix) + 0.5 * z - jnp.log(mass)
    share = domains // n_dp
    place = lax.broadcasted_iota(jnp.int32, (1, domains), 1)
    for j in range(share):
        out[j] = jnp.sum(jnp.where(place == dp * share + j, result, 0.0))

    everyone.wait_send()
    for i in range(chunks):
        exchange(i).wait_send()


def per_device(*args):
    (
        dense_act,
        dense_cot,
        dense_proj_in,
        dense_proj_out,
        expert_act,
        expert_cot,
        expert_proj_in,
        expert_proj_out,
        dense_valid,
        expert_valid,
        domain_ids,
        prior_mix,
    ) = args
    sizes = tuple(lax.axis_size(name) for name in ("dp", "expert", "tensor"))
    devices = sizes[0] * sizes[1] * sizes[2]
    layers, micro, tokens, feat = dense_act.shape
    half, width = dense_cot.shape[2:]
    experts, caps, hidden = expert_act.shape[1:]
    slots = expert_cot.shape[2]
    rank = dense_proj_in.shape[2]
    bf = dense_act.dtype
    chunks = micro + layers * micro
    n_loads = 1 + micro + layers * (1 + micro) + 5 + 2 * micro + layers * (1 + 2 * micro)
    return pl.pallas_call(
        functools.partial(kernel, sizes),
        out_shape=jax.ShapeDtypeStruct((prior_mix.shape[0] // sizes[0],), F32),
        in_specs=[pl.BlockSpec(memory_space=pl.ANY)] * len(args),
        out_specs=pl.BlockSpec(memory_space=pltpu.SMEM),
        scratch_shapes=[
            pltpu.VMEM((2, layers, micro, half, feat), bf),
            pltpu.VMEM((layers, micro, half, width), bf),
            pltpu.VMEM((layers, feat, rank), bf),
            pltpu.VMEM((layers, width, rank), bf),
            pltpu.VMEM((2, micro, experts, slots, hidden), bf),
            pltpu.VMEM((micro, experts, slots, width), bf),
            pltpu.VMEM((hidden, rank), bf),
            pltpu.VMEM((width, rank), bf),
            pltpu.VMEM(dense_valid.shape, F32),
            pltpu.VMEM(expert_valid.shape, F32),
            pltpu.SMEM(domain_ids.shape, jnp.int32),
            pltpu.VMEM(prior_mix.shape, F32),
            pltpu.VMEM((chunks, half, rank), F32),
            pltpu.VMEM((chunks, half, rank), F32),
            pltpu.VMEM((chunks, half, rank), F32),
            pltpu.VMEM((micro, 8, rank), F32),
            pltpu.VMEM((1, 128), F32),
            pltpu.VMEM((devices, 1, 128), F32),
            pltpu.SemaphoreType.REGULAR((4,)),
            pltpu.SemaphoreType.DMA((n_loads,)),
            pltpu.SemaphoreType.DMA((chunks,)),
            pltpu.SemaphoreType.DMA((chunks,)),
            pltpu.SemaphoreType.DMA,
            pltpu.SemaphoreType.DMA,
        ],
        compiler_params=pltpu.CompilerParams(
            collective_id=0, has_side_effects=True, vmem_limit_bytes=60 << 20
        ),
        name="align",
    )(*args)


def solution(mesh):
    placed = (
        P(None, "dp", "expert", "tensor"),
        P(None, "dp", ("expert", "tensor"), None),
        P(None, "tensor", None),
        P(),
        P("dp", "expert", None, "tensor"),
        P("dp", "expert", "tensor", None),
        P("tensor", None),
        P(),
        P(),
        P("expert", None, None),
        P("dp"),
        P(),
    )
    return jax.shard_map(per_device, mesh=mesh, in_specs=placed, out_specs=P("dp"), check_vma=False)
```

```python
import functools

import jax
import jax.numpy as jnp
from jax import lax
from jax.experimental import pallas as pl
from jax.experimental.pallas import tpu as pltpu
from jax.sharding import PartitionSpec as P

MESH = pl.DeviceIdType.MESH
F32 = jnp.float32
EXACT = lax.Precision.HIGHEST


def fold(product):
    rows, lanes = product.shape
    return jnp.sum(product.reshape(rows // 8, 8, lanes), axis=0)


def kernel(
    sizes,
    dense_act,
    dense_cot,
    dense_proj_in,
    dense_proj_out,
    expert_act,
    expert_cot,
    expert_proj_in,
    expert_proj_out,
    dense_valid,
    expert_valid,
    domain_ids,
    prior_mix,
    out,
    da,
    dc,
    pin,
    pout,
    ea,
    ec,
    epin,
    epout,
    dval,
    evalid,
    ids,
    prior,
    send,
    recv,
    wv,
    acc,
    row,
    rows,
    here,
    load_sem,
    send_sem,
    recv_sem,
    row_send_sem,
    row_recv_sem,
):
    n_dp, n_e, n_t = sizes
    devices = n_dp * n_e * n_t
    dp, ex, te = lax.axis_index("dp"), lax.axis_index("expert"), lax.axis_index("tensor")
    me = (dp * n_e + ex) * n_t + te
    layers, micro = dense_act.shape[0], dense_act.shape[1]
    half = dense_cot.shape[2]
    experts, slots = expert_cot.shape[1], expert_cot.shape[2]
    chunks = micro + layers * micro
    partner = {"tensor": 1 - te}

    ring = 4
    x, y, z = (dp % 2) * 2 + te, (dp // 2) % ring, dp // (2 * ring)

    def away(offset):
        dc, dx, dy, dz = offset
        cc = (ex + dc) % n_e
        xx, yy, zz = (x + dx) % ring, (y + dy) % ring, (z + dz) % ring
        return (((zz * ring + yy) * 2 + xx // n_t) * n_e + cc) * n_t + xx % n_t

    around = [(1, 0, 0, 0)]
    for axis in (1, 2, 3):
        for step in (1, ring - 1):
            around.append(tuple(step if k == axis else 0 for k in range(4)))
    lines = {
        axis: [tuple(step if k == axis else 0 for k in range(4)) for step in range(1, ring)]
        for axis in (1, 2, 3)
    }
    rounds = [around, lines[1], lines[2], around[:1]]

    def hello(semaphore, offsets):
        for offset in offsets:
            pl.semaphore_signal(
                semaphore, inc=1, device_id=away(offset), device_id_type=pl.DeviceIdType.LOGICAL
            )

    other = pl.multiple_of((1 - te) * half, half)
    mine = pl.multiple_of(te * half, half)
    e_other = pl.multiple_of((1 - te) * slots, slots)
    e_mine = pl.multiple_of(te * slots, slots)
    rest = pl.ds(1, micro - 1)
    plan = {
        "epin": (expert_proj_in, epin),
        "eao0": (expert_act.at[0, :, pl.ds(e_other, slots), :], ea.at[0, 0]),
        "eao": (expert_act.at[rest, :, pl.ds(e_other, slots), :], ea.at[0, rest]),
        "pin": (dense_proj_in, pin),
        ("dao", 0): (dense_act.at[0, :, pl.ds(other, half), :], da.at[0, 0]),
        ("dao", 1): (dense_act.at[1, :, pl.ds(other, half), :], da.at[0, 1]),
        "epout": (expert_proj_out, epout),
        "eam": (expert_act.at[:, :, pl.ds(e_mine, slots), :], ea.at[1]),
        "ec": (expert_cot, ec),
        "evalid": (expert_valid, evalid),
        "dval": (dense_valid, dval),
        "ids": (domain_ids, ids),
        "prior": (prior_mix, prior),
        "pout": (dense_proj_out, pout),
        ("dam", 0): (dense_act.at[0, :, pl.ds(mine, half), :], da.at[1, 0]),
        ("dc", 0): (dense_cot.at[0], dc.at[0]),
        ("dam", 1): (dense_act.at[1, :, pl.ds(mine, half), :], da.at[1, 1]),
        ("dc", 1): (dense_cot.at[1], dc.at[1]),
    }
    names = list(plan)
    loads = {
        name: pltpu.make_async_copy(*plan[name], load_sem.at[k]) for k, name in enumerate(names)
    }
    for name in names[:6]:
        loads[name].start()

    barrier = pltpu.get_barrier_semaphore()
    hello(barrier, around)

    def exchange(part, group):
        return pltpu.make_async_remote_copy(
            src_ref=send.at[part],
            dst_ref=recv.at[part],
            send_sem=send_sem,
            recv_sem=recv_sem.at[group],
            device_id=partner,
            device_id_type=MESH,
        )

    def project(block, weight):
        return jnp.dot(block, weight, preferred_element_type=F32)

    loads["epin"].wait()
    loads["eao0"].wait()
    head, tail = pl.ds(0, slots), pl.ds(slots, (experts - 1) * slots)
    send[0, head] = project(ea[0, 0, 0], epin[...])
    pl.semaphore_wait(barrier, len(around))
    exchange((0, head), 0).start()
    for name in names[6:]:
        loads[name].start()
    hello(here.at[0], rounds[0])
    send[0, tail] = project(ea[0, 0, 1:].reshape((experts - 1) * slots, -1), epin[...])
    exchange((0, tail), 0).start()
    loads["eao"].wait()
    for m in range(1, micro):
        send[m] = project(ea[0, m].reshape(experts * slots, -1), epin[...])
        exchange(m, 0).start()
    loads["pin"].wait()
    for l in range(layers):
        loads["dao", l].wait()
        for m in range(micro):
            i = micro + l * micro + m
            send[i] = project(da[0, l, m], pin[l])
            exchange(i, i // (chunks - 1)).start()

    for name in ("epout", "evalid", "dval", "eam", "ec"):
        loads[name].wait()
    for m in range(micro):
        pl.semaphore_wait(here.at[m], len(rounds[m]))
        if m + 1 < len(rounds):
            hello(here.at[m + 1], rounds[m + 1])
        u = project(ea[1, m].reshape(experts * slots, -1), epin[...])
        w = project(ec[m].reshape(experts * slots, -1), epout[...])
        parts = [
            lax.dot_general(
                w[e * slots : (e + 1) * slots],
                evalid[e],
                (((1,), (1,)), ((), ())),
                precision=EXACT,
                preferred_element_type=F32,
            )
            for e in range(experts)
        ]
        wv_i = jnp.concatenate(parts, axis=0)
        wv[m] = wv_i
        acc[m] = fold(u * wv_i)
    loads["pout"].wait()
    for l in range(layers):
        loads["dam", l].wait()
        loads["dc", l].wait()
        for m in range(micro):
            i = micro + l * micro + m
            u = project(da[1, l, m], pin[l])
            w = project(dc[l, m], pout[l])
            wv_i = lax.dot_general(
                w, dval[l], (((1,), (1,)), ((), ())), precision=EXACT, preferred_element_type=F32
            )
            wv[i] = wv_i
            acc[m] += fold(u * wv_i)
    loads["ids"].wait()
    loads["prior"].wait()
    domains = prior_mix.shape[0]
    share = domains // n_dp
    mix = prior[...].reshape(1, domains)
    log_mix = jnp.log(mix)
    place = lax.broadcasted_iota(jnp.int32, (1, domains), 1)
    lane = lax.broadcasted_iota(jnp.int32, (1, 128), 1)

    def own(values, j):
        return jnp.sum(jnp.where(place == dp * share + j, values, 0.0), axis=1, keepdims=True)

    early = pl.ds(0, chunks - 1)
    exchange(early, 0).wait_recv()
    sums = []
    for m in range(micro):
        s = acc[m]
        for i in range(m, chunks - 1, micro):
            s += fold(recv[i] * wv[i])
        sums.append(s)
    exchange(chunks - 1, 1).wait_recv()
    sums[micro - 1] += fold(recv[chunks - 1] * wv[chunks - 1])
    mine_row = jnp.zeros((1, 128), F32)
    for m in range(micro):
        s = jnp.sum(jnp.sum(sums[m], axis=0, keepdims=True), axis=1, keepdims=True)
        mine_row += jnp.where(lane == ids[m], s, 0.0)

    row[...] = mine_row
    rows[me] = mine_row

    hops = lambda offset: sum(min(d, n - d) for d, n in zip(offset, (2, ring, ring, ring)))
    offsets = [
        (dc, dx, dy, dz)
        for dc in range(n_e)
        for dx in range(ring)
        for dy in range(ring)
        for dz in range(ring)
    ][1:]
    offsets.sort(key=hops, reverse=True)
    targets = [away(offset) for offset in offsets]
    for k, first in enumerate((0, n_t)):
        first = jnp.where(me == first, targets[k], first)
        targets[k + 1 :] = [jnp.where(t == first, targets[k], t) for t in targets[k + 1 :]]
        targets[k] = first
    for target in targets:
        pltpu.make_async_remote_copy(
            src_ref=row,
            dst_ref=rows.at[me],
            send_sem=row_send_sem,
            recv_sem=row_recv_sem,
            device_id=target,
            device_id_type=pl.DeviceIdType.LOGICAL,
        ).start()
    everyone = pltpu.make_async_remote_copy(
        src_ref=rows.at[pl.ds(0, devices - 1)],
        dst_ref=rows.at[pl.ds(0, devices - 1)],
        send_sem=row_send_sem,
        recv_sem=row_recv_sem,
        device_id=partner,
        device_id_type=MESH,
    )
    everyone.wait_recv()
    total = jnp.sum(rows.reshape(devices, 128)[...], axis=0, keepdims=True)[:, :domains]
    spread = jnp.sqrt(jnp.sum(total * total, axis=1, keepdims=True) / domains + 1e-06)
    mass = jnp.sum(mix * jnp.exp(0.5 * (total / spread)), axis=1, keepdims=True)
    common = jnp.log(mass)
    answer = jnp.zeros((1, 128), F32)
    for j in range(share):
        picked = own(log_mix, j) + 0.5 * (own(total, j) / spread) - common
        answer = jnp.where(lane == j, picked, answer)
    out[...] = answer[:, :share].reshape(share)

    everyone.wait_send()
    exchange(pl.ds(0, chunks), 0).wait_send()


def per_device(*args):
    (
        dense_act,
        dense_cot,
        dense_proj_in,
        dense_proj_out,
        expert_act,
        expert_cot,
        expert_proj_in,
        expert_proj_out,
        dense_valid,
        expert_valid,
        domain_ids,
        prior_mix,
    ) = args
    sizes = tuple(lax.axis_size(name) for name in ("dp", "expert", "tensor"))
    devices = sizes[0] * sizes[1] * sizes[2]
    layers, micro, tokens, feat = dense_act.shape
    half, width = dense_cot.shape[2:]
    experts, caps, hidden = expert_act.shape[1:]
    slots = expert_cot.shape[2]
    rank = dense_proj_in.shape[2]
    bf = dense_act.dtype
    chunks = micro + layers * micro
    n_loads = 18
    return pl.pallas_call(
        functools.partial(kernel, sizes),
        out_shape=jax.ShapeDtypeStruct((prior_mix.shape[0] // sizes[0],), F32),
        in_specs=[pl.BlockSpec(memory_space=pl.ANY)] * len(args),
        out_specs=pl.BlockSpec(memory_space=pltpu.VMEM),
        scratch_shapes=[
            pltpu.VMEM((2, layers, micro, half, feat), bf),
            pltpu.VMEM((layers, micro, half, width), bf),
            pltpu.VMEM((layers, feat, rank), bf),
            pltpu.VMEM((layers, width, rank), bf),
            pltpu.VMEM((2, micro, experts, slots, hidden), bf),
            pltpu.VMEM((micro, experts, slots, width), bf),
            pltpu.VMEM((hidden, rank), bf),
            pltpu.VMEM((width, rank), bf),
            pltpu.VMEM(dense_valid.shape, F32),
            pltpu.VMEM(expert_valid.shape, F32),
            pltpu.SMEM(domain_ids.shape, jnp.int32),
            pltpu.VMEM(prior_mix.shape, F32),
            pltpu.VMEM((chunks, half, rank), F32),
            pltpu.VMEM((chunks, half, rank), F32),
            pltpu.VMEM((chunks, half, rank), F32),
            pltpu.VMEM((micro, 8, rank), F32),
            pltpu.VMEM((1, 128), F32),
            pltpu.VMEM((devices, 1, 128), F32),
            pltpu.SemaphoreType.REGULAR((4,)),
            pltpu.SemaphoreType.DMA((n_loads,)),
            pltpu.SemaphoreType.DMA,
            pltpu.SemaphoreType.DMA((2,)),
            pltpu.SemaphoreType.DMA,
            pltpu.SemaphoreType.DMA,
        ],
        compiler_params=pltpu.CompilerParams(
            collective_id=0, has_side_effects=True, vmem_limit_bytes=56551424
        ),
        name="align",
    )(*args)


def solution(mesh):
    placed = (
        P(None, "dp", "expert", "tensor"),
        P(None, "dp", ("expert", "tensor"), None),
        P(None, "tensor", None),
        P(),
        P("dp", "expert", None, "tensor"),
        P("dp", "expert", "tensor", None),
        P("tensor", None),
        P(),
        P(),
        P("expert", None, None),
        P("dp"),
        P(),
    )
    return jax.shard_map(per_device, mesh=mesh, in_specs=placed, out_specs=P("dp"), check_vma=False)
```

```python
import functools

import jax
import jax.numpy as jnp
from jax import lax
from jax.experimental import pallas as pl
from jax.experimental.pallas import tpu as pltpu
from jax.sharding import PartitionSpec as P

MESH = pl.DeviceIdType.MESH
F32 = jnp.float32
HOLD = 8
KEEP = 6
SPARE = 3
EXACT = lax.Precision.HIGHEST


def fold(product):
    rows, lanes = product.shape
    return jnp.sum(product.reshape(rows // 8, 8, lanes), axis=0)


def kernel(
    sizes,
    dense_act,
    dense_cot,
    dense_proj_in,
    dense_proj_out,
    expert_act,
    expert_cot,
    expert_proj_in,
    expert_proj_out,
    dense_valid,
    expert_valid,
    domain_ids,
    prior_mix,
    out,
    da,
    dc,
    pin,
    pout,
    ea,
    ec,
    epin,
    epout,
    dval,
    evalid,
    ids,
    prior,
    send,
    recv,
    wv,
    acc,
    row,
    rows,
    relay_a,
    relay_b,
    relay_sem,
    here,
    load_sem,
    send_sem,
    recv_sem,
    row_send_sem,
    row_recv_sem,
):
    n_dp, n_e, n_t = sizes
    devices = n_dp * n_e * n_t
    dp, ex, te = lax.axis_index("dp"), lax.axis_index("expert"), lax.axis_index("tensor")
    me = (dp * n_e + ex) * n_t + te
    layers, micro = dense_act.shape[0], dense_act.shape[1]
    half = dense_cot.shape[2]
    experts, slots = expert_cot.shape[1], expert_cot.shape[2]
    chunks = micro + layers * micro
    partner = {"tensor": 1 - te}

    ring = 4
    x, y, z = (dp % 2) * 2 + te, (dp // 2) % ring, dp // (2 * ring)

    last = ring - 1

    def number(cc, xx, yy, zz):
        return (((zz * ring + yy) * 2 + xx // n_t) * n_e + cc) * n_t + xx % n_t

    def away(offset):
        dc, dx, dy, dz = offset
        return number((ex + dc) % n_e, (x + dx) % ring, (y + dy) % ring, (z + dz) % ring)

    def signal(semaphore, target):
        pl.semaphore_signal(
            semaphore, inc=1, device_id=target, device_id_type=pl.DeviceIdType.LOGICAL
        )

    def signal_if(condition, semaphore, target):
        @pl.when(condition)
        def _():
            signal(semaphore, target)

    age = y + 2 * z
    mate, sibling, across = number(ex, x + 1 - 2 * te, y, z), number(1 - ex, x, y, z), number(ex, last - x, y, z)
    mirror = number(ex, x, last - y, last - z)
    up_y, down_y = number(ex, x, (y + 1) % ring, z), number(ex, x, (y + last) % ring, z)
    up_z, down_z = number(ex, x, y, (z + 1) % ring), number(ex, x, y, (z + last) % ring)
    giver2, giver1 = age >= 8, age >= 6
    helper2, helper1 = age <= 1, age <= 3

    def hello(k):
        if k == 0:
            semaphore = pltpu.get_barrier_semaphore()
            signal(semaphore, mate)
            signal(semaphore, sibling)
            signal_if(x < n_t, semaphore, across)
            signal_if(helper1, semaphore, mirror)
        else:
            semaphore = here.at[k - 1]
        if k == 1:
            signal_if(x >= n_t, semaphore, across)
        if k in (2, 3):
            for target in (mate, sibling, across):
                signal(semaphore, target)
        if k in (0, 2, 3):
            signal_if(y < last, semaphore, up_y)
            signal_if(z < last, semaphore, up_z)
        if k in (1, 2, 3):
            signal_if(y > 0, semaphore, down_y)
            signal_if(z > 0, semaphore, down_z)
        if k in (4, 5):
            for step in range(1, ring):
                signal(semaphore, away((0, step, 0, 0) if k == 4 else (0, 0, step, 0)))
        if k == 6:
            signal(semaphore, sibling)

    from_below = (y + last) // ring + (z + last) // ring
    from_above = 2 - y // last - z // last
    heard = {
        0: 2 + from_below + x // n_t + age // 6,
        1: from_above + 1 - x // n_t,
        2: 3 + from_below + from_above,
        3: 3 + from_below + from_above,
        4: ring - 1,
        5: ring - 1,
        6: 1,
    }

    def listen(k):
        semaphore = pltpu.get_barrier_semaphore() if k == 0 else here.at[k - 1]
        if k == 1:

            @pl.when(heard[k] > 0)
            def _():
                pl.semaphore_wait(semaphore, heard[k])

        else:
            pl.semaphore_wait(semaphore, heard[k])

    other = pl.multiple_of((1 - te) * half, half)
    mine = pl.multiple_of(te * half, half)
    e_other = pl.multiple_of((1 - te) * slots, slots)
    e_mine = pl.multiple_of(te * slots, slots)
    rest = pl.ds(1, micro - 1)
    plan = {
        "epin": (expert_proj_in, epin),
        "eao0": (expert_act.at[0, :, pl.ds(e_other, slots), :], ea.at[0, 0]),
        "eao": (expert_act.at[rest, :, pl.ds(e_other, slots), :], ea.at[0, rest]),
        "pin": (dense_proj_in, pin),
        ("dao", 0): (dense_act.at[0, :, pl.ds(other, half), :], da.at[0, 0]),
        ("dao", 1): (dense_act.at[1, :, pl.ds(other, half), :], da.at[0, 1]),
        "epout": (expert_proj_out, epout),
        "eam": (expert_act.at[:, :, pl.ds(e_mine, slots), :], ea.at[1]),
        "ec": (expert_cot, ec),
        "evalid": (expert_valid, evalid),
        "dval": (dense_valid, dval),
        "ids": (domain_ids, ids),
        "prior": (prior_mix, prior),
        "pout": (dense_proj_out, pout),
        ("dam", 0): (dense_act.at[0, :, pl.ds(mine, half), :], da.at[1, 0]),
        ("dc", 0): (dense_cot.at[0], dc.at[0]),
        ("dam", 1): (dense_act.at[1, :, pl.ds(mine, half), :], da.at[1, 1]),
        ("dc", 1): (dense_cot.at[1], dc.at[1]),
    }
    names = list(plan)
    loads = {
        name: pltpu.make_async_copy(*plan[name], load_sem.at[k]) for k, name in enumerate(names)
    }
    for name in names[:6]:
        loads[name].start()

    hello(0)

    def exchange(part, group):
        return pltpu.make_async_remote_copy(
            src_ref=send.at[part],
            dst_ref=recv.at[part],
            send_sem=send_sem,
            recv_sem=recv_sem.at[group],
            device_id=partner,
            device_id_type=MESH,
        )

    def project(block, weight):
        return jnp.dot(block, weight, preferred_element_type=F32)

    halves = (pl.ds(0, half // 2), pl.ds(half // 2, half // 2))

    def hop(source, target, sent, arrived, device):
        return pltpu.make_async_remote_copy(
            src_ref=source,
            dst_ref=target,
            send_sem=sent,
            recv_sem=arrived,
            device_id=device,
            device_id_type=pl.DeviceIdType.LOGICAL,
        )

    def give(k):
        return hop(send.at[SPARE, halves[k]], relay_a.at[k], send_sem, relay_sem.at[0, k], mirror)

    def pass_on(k):
        return hop(relay_a.at[k], relay_b.at[k], relay_sem.at[1, k], relay_sem.at[2, k], mate)

    def deliver(k):
        return hop(
            relay_b.at[k], recv.at[SPARE, halves[k]], relay_sem.at[3, k], recv_sem.at[0], mirror
        )

    loads["epin"].wait()
    loads["eao0"].wait()
    head, tail = pl.ds(0, slots), pl.ds(slots, (experts - 1) * slots)
    send[0, head] = project(ea[0, 0, 0], epin[...])
    listen(0)
    exchange((0, head), 0).start()
    for name in names[6:]:
        loads[name].start()
    hello(1)
    send[0, tail] = project(ea[0, 0, 1:].reshape((experts - 1) * slots, -1), epin[...])
    exchange((0, tail), 0).start()
    loads["eao"].wait()
    send[SPARE] = project(ea[0, SPARE].reshape(experts * slots, -1), epin[...])
    for k, giver in enumerate((giver1, giver2)):

        @pl.when(giver)
        def _():
            give(k).start()

        @pl.when(jnp.logical_not(giver))
        def _():
            exchange((SPARE, halves[k]), 0).start()

    def start(i):
        exchange(i, i // (chunks - 1)).start()

    order = [i for i in range(1, chunks) if i != SPARE]

    def ready(i):
        if i < KEEP:

            @pl.when(jnp.logical_or(helper1, ex == 0))
            def _():
                start(i)

        elif i <= HOLD:

            @pl.when(jnp.logical_and(jnp.logical_not(helper1), ex == 0))
            def _():
                start(i)

        else:

            @pl.when(jnp.logical_not(helper1))
            def _():
                start(i)

        if i == HOLD:

            @pl.when(jnp.logical_and(jnp.logical_not(helper1), ex != 0))
            def _():
                for j in order:
                    if j <= HOLD:
                        start(j)

    for m in range(1, micro):
        if m != SPARE:
            send[m] = project(ea[0, m].reshape(experts * slots, -1), epin[...])
            ready(m)
    loads["pin"].wait()
    for l in range(layers):
        loads["dao", l].wait()
        for m in range(micro):
            i = micro + l * micro + m
            send[i] = project(da[0, l, m], pin[l])
            ready(i)

    meetings = {0: 1, 2: 2, 4: 3, 5: 4, 6: 5, 8: 6}

    def meet(step):
        if step in meetings:
            listen(meetings[step])
            if meetings[step] < 6:
                hello(meetings[step] + 1)

    for name in ("epout", "evalid", "dval", "eam", "ec"):
        loads[name].wait()
    for m in range(micro):
        meet(m)
        u = project(ea[1, m].reshape(experts * slots, -1), epin[...])
        w = project(ec[m].reshape(experts * slots, -1), epout[...])
        parts = [
            lax.dot_general(
                w[e * slots : (e + 1) * slots],
                evalid[e],
                (((1,), (1,)), ((), ())),
                precision=EXACT,
                preferred_element_type=F32,
            )
            for e in range(experts)
        ]
        wv_i = jnp.concatenate(parts, axis=0)
        wv[m] = wv_i
        acc[m] = fold(u * wv_i)
        if m == 1:
            for k, helper in enumerate((helper1, helper2)):

                @pl.when(helper)
                def _():
                    give(k).wait_recv()
                    pass_on(k).start()

            @pl.when(helper1)
            def _():
                for j in order:
                    if j >= KEEP:
                        start(j)

    loads["pout"].wait()
    for l in range(layers):
        loads["dam", l].wait()
        loads["dc", l].wait()
        for m in range(micro):
            i = micro + l * micro + m
            meet(i)
            u = project(da[1, l, m], pin[l])
            w = project(dc[l, m], pout[l])
            wv_i = lax.dot_general(
                w, dval[l], (((1,), (1,)), ((), ())), precision=EXACT, preferred_element_type=F32
            )
            wv[i] = wv_i
            acc[m] += fold(u * wv_i)
            if i == 7:
                for k, helper in enumerate((helper1, helper2)):

                    @pl.when(helper)
                    def _():
                        pass_on(k).wait_recv()
                        deliver(k).start()

    loads["ids"].wait()
    loads["prior"].wait()
    domains = prior_mix.shape[0]
    share = domains // n_dp
    mix = prior[...].reshape(1, domains)
    log_mix = jnp.log(mix)
    place = lax.broadcasted_iota(jnp.int32, (1, domains), 1)
    lane = lax.broadcasted_iota(jnp.int32, (1, 128), 1)

    def own(values, j):
        return jnp.sum(jnp.where(place == dp * share + j, values, 0.0), axis=1, keepdims=True)

    early = pl.ds(0, chunks - 1)
    exchange(early, 0).wait_recv()
    sums = []
    for m in range(micro):
        s = acc[m]
        for i in range(m, chunks - 1, micro):
            s += fold(recv[i] * wv[i])
        sums.append(s)
    exchange(chunks - 1, 1).wait_recv()
    sums[micro - 1] += fold(recv[chunks - 1] * wv[chunks - 1])
    mine_row = jnp.zeros((1, 128), F32)
    for m in range(micro):
        s = jnp.sum(jnp.sum(sums[m], axis=0, keepdims=True), axis=1, keepdims=True)
        mine_row += jnp.where(lane == ids[m], s, 0.0)

    row[...] = mine_row
    rows[me] = mine_row

    hops = lambda offset: sum(min(d, n - d) for d, n in zip(offset, (2, ring, ring, ring)))
    offsets = [
        (dc, dx, dy, dz)
        for dc in range(n_e)
        for dx in range(ring)
        for dy in range(ring)
        for dz in range(ring)
    ][1:]
    offsets.sort(key=hops, reverse=True)
    targets = [away(offset) for offset in offsets]
    for k, first in enumerate((n_t, 0)):
        first = jnp.where(me == first, targets[k], first)
        targets[k + 1 :] = [jnp.where(t == first, targets[k], t) for t in targets[k + 1 :]]
        targets[k] = first
    for target in targets:
        pltpu.make_async_remote_copy(
            src_ref=row,
            dst_ref=rows.at[me],
            send_sem=row_send_sem,
            recv_sem=row_recv_sem,
            device_id=target,
            device_id_type=pl.DeviceIdType.LOGICAL,
        ).start()
    everyone = pltpu.make_async_remote_copy(
        src_ref=rows.at[pl.ds(0, devices - 1)],
        dst_ref=rows.at[pl.ds(0, devices - 1)],
        send_sem=row_send_sem,
        recv_sem=row_recv_sem,
        device_id=partner,
        device_id_type=MESH,
    )
    everyone.wait_recv()
    total = jnp.sum(rows.reshape(devices, 128)[...], axis=0, keepdims=True)[:, :domains]
    spread = jnp.sqrt(jnp.sum(total * total, axis=1, keepdims=True) / domains + 1e-06)
    mass = jnp.sum(mix * jnp.exp(0.5 * (total / spread)), axis=1, keepdims=True)
    common = jnp.log(mass)
    answer = jnp.zeros((1, 128), F32)
    for j in range(share):
        picked = own(log_mix, j) + 0.5 * (own(total, j) / spread) - common
        answer = jnp.where(lane == j, picked, answer)
    out[...] = answer[:, :share].reshape(share)

    everyone.wait_send()
    exchange(pl.ds(0, chunks), 0).wait_send()
    for k, helper in enumerate((helper1, helper2)):

        @pl.when(helper)
        def _():
            pass_on(k).wait_send()
            deliver(k).wait_send()


def per_device(*args):
    (
        dense_act,
        dense_cot,
        dense_proj_in,
        dense_proj_out,
        expert_act,
        expert_cot,
        expert_proj_in,
        expert_proj_out,
        dense_valid,
        expert_valid,
        domain_ids,
        prior_mix,
    ) = args
    sizes = tuple(lax.axis_size(name) for name in ("dp", "expert", "tensor"))
    devices = sizes[0] * sizes[1] * sizes[2]
    layers, micro, tokens, feat = dense_act.shape
    half, width = dense_cot.shape[2:]
    experts, caps, hidden = expert_act.shape[1:]
    slots = expert_cot.shape[2]
    rank = dense_proj_in.shape[2]
    bf = dense_act.dtype
    chunks = micro + layers * micro
    n_loads = 18
    return pl.pallas_call(
        functools.partial(kernel, sizes),
        out_shape=jax.ShapeDtypeStruct((prior_mix.shape[0] // sizes[0],), F32),
        in_specs=[pl.BlockSpec(memory_space=pl.ANY)] * len(args),
        out_specs=pl.BlockSpec(memory_space=pltpu.VMEM),
        scratch_shapes=[
            pltpu.VMEM((2, layers, micro, half, feat), bf),
            pltpu.VMEM((layers, micro, half, width), bf),
            pltpu.VMEM((layers, feat, rank), bf),
            pltpu.VMEM((layers, width, rank), bf),
            pltpu.VMEM((2, micro, experts, slots, hidden), bf),
            pltpu.VMEM((micro, experts, slots, width), bf),
            pltpu.VMEM((hidden, rank), bf),
            pltpu.VMEM((width, rank), bf),
            pltpu.VMEM(dense_valid.shape, F32),
            pltpu.VMEM(expert_valid.shape, F32),
            pltpu.SMEM(domain_ids.shape, jnp.int32),
            pltpu.VMEM(prior_mix.shape, F32),
            pltpu.VMEM((chunks, half, rank), F32),
            pltpu.VMEM((chunks, half, rank), F32),
            pltpu.VMEM((chunks, half, rank), F32),
            pltpu.VMEM((micro, 8, rank), F32),
            pltpu.VMEM((1, 128), F32),
            pltpu.VMEM((devices, 1, 128), F32),
            pltpu.VMEM((2, half // 2, rank), F32),
            pltpu.VMEM((2, half // 2, rank), F32),
            pltpu.SemaphoreType.DMA((4, 2)),
            pltpu.SemaphoreType.REGULAR((6,)),
            pltpu.SemaphoreType.DMA((n_loads,)),
            pltpu.SemaphoreType.DMA,
            pltpu.SemaphoreType.DMA((2,)),
            pltpu.SemaphoreType.DMA,
            pltpu.SemaphoreType.DMA,
        ],
        compiler_params=pltpu.CompilerParams(
            collective_id=0, has_side_effects=True, vmem_limit_bytes=56551424
        ),
        name="align",
    )(*args)


def solution(mesh):
    placed = (
        P(None, "dp", "expert", "tensor"),
        P(None, "dp", ("expert", "tensor"), None),
        P(None, "tensor", None),
        P(),
        P("dp", "expert", None, "tensor"),
        P("dp", "expert", "tensor", None),
        P("tensor", None),
        P(),
        P(),
        P("expert", None, None),
        P("dp"),
        P(),
    )
    return jax.shard_map(per_device, mesh=mesh, in_specs=placed, out_specs=P("dp"), check_vma=False)
```

```python
import functools

import jax
import jax.numpy as jnp
from jax import lax
from jax.experimental import pallas as pl
from jax.experimental.pallas import tpu as pltpu
from jax.sharding import PartitionSpec as P

MESH = pl.DeviceIdType.MESH
F32 = jnp.float32
HOLD = 10
KEEP = 6
SPARE = (3, 2)
PASS = 3
DELIVER = (6, 7,)
LIMITS = (21, 26)
EXACT = lax.Precision.HIGHEST


def fold(product):
    rows, lanes = product.shape
    return jnp.sum(product.reshape(rows // 8, 8, lanes), axis=0)


def kernel(
    sizes,
    dense_act,
    dense_cot,
    dense_proj_in,
    dense_proj_out,
    expert_act,
    expert_cot,
    expert_proj_in,
    expert_proj_out,
    dense_valid,
    expert_valid,
    domain_ids,
    prior_mix,
    out,
    da,
    dc,
    pin,
    pout,
    ea,
    ec,
    epin,
    epout,
    dval,
    evalid,
    ids,
    prior,
    send,
    recv,
    wv,
    acc,
    row,
    rows,
    relay_a,
    relay_b,
    relay_sem,
    here,
    load_sem,
    send_sem,
    recv_sem,
    row_send_sem,
    row_recv_sem,
):
    n_dp, n_e, n_t = sizes
    devices = n_dp * n_e * n_t
    dp, ex, te = lax.axis_index("dp"), lax.axis_index("expert"), lax.axis_index("tensor")
    me = (dp * n_e + ex) * n_t + te
    layers, micro = dense_act.shape[0], dense_act.shape[1]
    half = dense_cot.shape[2]
    experts, slots = expert_cot.shape[1], expert_cot.shape[2]
    chunks = micro + layers * micro
    partner = {"tensor": 1 - te}

    ring = 4
    x, y, z = (dp % 2) * 2 + te, (dp // 2) % ring, dp // (2 * ring)

    last = ring - 1

    def number(cc, xx, yy, zz):
        return (((zz * ring + yy) * 2 + xx // n_t) * n_e + cc) * n_t + xx % n_t

    def away(offset):
        dc, dx, dy, dz = offset
        return number((ex + dc) % n_e, (x + dx) % ring, (y + dy) % ring, (z + dz) % ring)

    def signal(semaphore, target):
        pl.semaphore_signal(
            semaphore, inc=1, device_id=target, device_id_type=pl.DeviceIdType.LOGICAL
        )

    def signal_if(condition, semaphore, target):
        @pl.when(condition)
        def _():
            signal(semaphore, target)

    mate, sibling, across = number(ex, x + 1 - 2 * te, y, z), number(1 - ex, x, y, z), number(ex, last - x, y, z)
    mirror = number(ex, last - x, last - y, last - z)
    up_y, down_y = number(ex, x, (y + 1) % ring, z), number(ex, x, (y + last) % ring, z)
    up_z, down_z = number(ex, x, y, (z + 1) % ring), number(ex, x, y, (z + last) % ring)

    def late(xx, yy, zz):
        return 5 * (xx // n_t) + 5 * yy - 4 * (yy // last) + 6 * zz - 4 * (zz // last)

    mine_late, mirror_late = late(x, y, z), late(last - x, last - y, last - z)
    givers = [mine_late >= limit for limit in LIMITS]
    helpers = [mirror_late >= limit for limit in LIMITS]
    helping = helpers[0]

    def hello(k):
        if k == 0:
            semaphore = pltpu.get_barrier_semaphore()
            signal(semaphore, mate)
            signal(semaphore, sibling)
            signal_if(x < n_t, semaphore, across)
            signal_if(helping, semaphore, mirror)
        else:
            semaphore = here.at[k - 1]
        if k == 1:
            signal_if(x >= n_t, semaphore, across)
        if k in (2, 3):
            for target in (mate, sibling, across):
                signal(semaphore, target)
        if k in (0, 2, 3):
            signal_if(y < last, semaphore, up_y)
            signal_if(z < last, semaphore, up_z)
        if k in (1, 2, 3):
            signal_if(y > 0, semaphore, down_y)
            signal_if(z > 0, semaphore, down_z)
        if k in (4, 5):
            for step in range(1, ring):
                signal(semaphore, away((0, step, 0, 0) if k == 4 else (0, 0, step, 0)))
        if k == 6:
            signal(semaphore, sibling)

    from_below = (y + last) // ring + (z + last) // ring
    from_above = 2 - y // last - z // last
    heard = {
        0: 2 + from_below + x // n_t + jnp.where(givers[0], 1, 0),
        1: from_above + 1 - x // n_t,
        2: 3 + from_below + from_above,
        3: 3 + from_below + from_above,
        4: ring - 1,
        5: ring - 1,
        6: 1,
    }

    def listen(k):
        semaphore = pltpu.get_barrier_semaphore() if k == 0 else here.at[k - 1]
        if k == 1:

            @pl.when(heard[k] > 0)
            def _():
                pl.semaphore_wait(semaphore, heard[k])

        else:
            pl.semaphore_wait(semaphore, heard[k])

    other = pl.multiple_of((1 - te) * half, half)
    mine = pl.multiple_of(te * half, half)
    e_other = pl.multiple_of((1 - te) * slots, slots)
    e_mine = pl.multiple_of(te * slots, slots)
    rest = pl.ds(1, micro - 1)
    plan = {
        "epin": (expert_proj_in, epin),
        "eao0": (expert_act.at[0, :, pl.ds(e_other, slots), :], ea.at[0, 0]),
        "eao": (expert_act.at[rest, :, pl.ds(e_other, slots), :], ea.at[0, rest]),
        "pin": (dense_proj_in, pin),
        ("dao", 0): (dense_act.at[0, :, pl.ds(other, half), :], da.at[0, 0]),
        ("dao", 1): (dense_act.at[1, :, pl.ds(other, half), :], da.at[0, 1]),
        "epout": (expert_proj_out, epout),
        "eam": (expert_act.at[:, :, pl.ds(e_mine, slots), :], ea.at[1]),
        "ec": (expert_cot, ec),
        "evalid": (expert_valid, evalid),
        "dval": (dense_valid, dval),
        "ids": (domain_ids, ids),
        "prior": (prior_mix, prior),
        "pout": (dense_proj_out, pout),
        ("dam", 0): (dense_act.at[0, :, pl.ds(mine, half), :], da.at[1, 0]),
        ("dc", 0): (dense_cot.at[0], dc.at[0]),
        ("dam", 1): (dense_act.at[1, :, pl.ds(mine, half), :], da.at[1, 1]),
        ("dc", 1): (dense_cot.at[1], dc.at[1]),
    }
    names = list(plan)
    loads = {
        name: pltpu.make_async_copy(*plan[name], load_sem.at[k]) for k, name in enumerate(names)
    }
    for name in names[:6]:
        loads[name].start()

    hello(0)

    def exchange(part, group):
        return pltpu.make_async_remote_copy(
            src_ref=send.at[part],
            dst_ref=recv.at[part],
            send_sem=send_sem,
            recv_sem=recv_sem.at[group],
            device_id=partner,
            device_id_type=MESH,
        )

    def project(block, weight):
        return jnp.dot(block, weight, preferred_element_type=F32)

    halves = (pl.ds(0, half // 2), pl.ds(half // 2, half // 2))
    units = [(i, part) for i in SPARE for part in halves][: len(LIMITS)]

    def hop(source, target, sent, arrived, device):
        return pltpu.make_async_remote_copy(
            src_ref=source,
            dst_ref=target,
            send_sem=sent,
            recv_sem=arrived,
            device_id=device,
            device_id_type=pl.DeviceIdType.LOGICAL,
        )

    def give(k):
        return hop(send.at[units[k]], relay_a.at[k], send_sem, relay_sem.at[0, k], mirror)

    def pass_on(k):
        return hop(relay_a.at[k], relay_b.at[k], relay_sem.at[1, k], relay_sem.at[2, k], mate)

    def deliver(k):
        return hop(
            relay_b.at[k], recv.at[units[k]], relay_sem.at[3, k], recv_sem.at[0], mirror
        )

    loads["epin"].wait()
    loads["eao0"].wait()
    head, tail = pl.ds(0, slots), pl.ds(slots, (experts - 1) * slots)
    send[0, head] = project(ea[0, 0, 0], epin[...])
    listen(0)
    exchange((0, head), 0).start()
    for name in names[6:]:
        loads[name].start()
    hello(1)
    send[0, tail] = project(ea[0, 0, 1:].reshape((experts - 1) * slots, -1), epin[...])
    exchange((0, tail), 0).start()
    loads["eao"].wait()
    for i in SPARE:
        send[i] = project(ea[0, i].reshape(experts * slots, -1), epin[...])
        for part in halves:
            if (i, part) not in units:

                @pl.when(ex == 0)
                def _():
                    exchange((i, part), 0).start()

                continue
            k = units.index((i, part))

            @pl.when(givers[k])
            def _():
                give(k).start()

            direct = jnp.logical_not(givers[k])

            @pl.when(jnp.logical_and(direct, ex == 0) if i != SPARE[0] else direct)
            def _():
                exchange(units[k], 0).start()

    def start(i):
        exchange(i, i // (chunks - 1)).start()

    order = [i for i in range(1, chunks) if i not in SPARE]

    def ready(i):
        if i < KEEP:

            @pl.when(ex == 0)
            def _():
                start(i)

        elif i <= HOLD:

            @pl.when(jnp.logical_and(jnp.logical_not(helping), ex == 0))
            def _():
                start(i)

        else:

            @pl.when(jnp.logical_not(helping))
            def _():
                start(i)

        if i == HOLD:

            @pl.when(ex != 0)
            def _():
                for j in order:
                    if j < KEEP:
                        start(j)

            for j in SPARE[1:]:
                for part in halves:
                    held = ex != 0
                    if (j, part) in units:
                        giving = givers[units.index((j, part))]
                        held = jnp.logical_and(held, jnp.logical_not(giving))

                    @pl.when(held)
                    def _():
                        exchange((j, part), 0).start()

            @pl.when(jnp.logical_and(jnp.logical_not(helping), ex != 0))
            def _():
                for j in order:
                    if KEEP <= j <= HOLD:
                        start(j)

    for m in range(1, micro):
        if m not in SPARE:
            send[m] = project(ea[0, m].reshape(experts * slots, -1), epin[...])
            ready(m)
    loads["pin"].wait()
    for l in range(layers):
        loads["dao", l].wait()
        for m in range(micro):
            i = micro + l * micro + m
            send[i] = project(da[0, l, m], pin[l])
            ready(i)

    meetings = {0: 1, 2: 2, 4: 3, 5: 4, 6: 5, 8: 6}

    def meet(step):
        if step in meetings:
            listen(meetings[step])
            if meetings[step] < 6:
                hello(meetings[step] + 1)

    def relay(step):
        if step == PASS:
            for k, helper in enumerate(helpers):

                @pl.when(helper)
                def _():
                    give(k).wait_recv()
                    pass_on(k).start()

            @pl.when(helping)
            def _():
                for j in order:
                    if j >= KEEP:
                        start(j)

        for k, helper in enumerate(helpers):
            if step == DELIVER[k]:

                @pl.when(helper)
                def _():
                    pass_on(k).wait_recv()
                    deliver(k).start()

    for name in ("epout", "evalid", "dval", "eam", "ec"):
        loads[name].wait()
    for m in range(micro):
        meet(m)
        u = project(ea[1, m].reshape(experts * slots, -1), epin[...])
        w = project(ec[m].reshape(experts * slots, -1), epout[...])
        parts = [
            lax.dot_general(
                w[e * slots : (e + 1) * slots],
                evalid[e],
                (((1,), (1,)), ((), ())),
                precision=EXACT,
                preferred_element_type=F32,
            )
            for e in range(experts)
        ]
        wv_i = jnp.concatenate(parts, axis=0)
        wv[m] = wv_i
        acc[m] = fold(u * wv_i)
        relay(m)
    loads["pout"].wait()
    for l in range(layers):
        loads["dam", l].wait()
        loads["dc", l].wait()
        for m in range(micro):
            i = micro + l * micro + m
            meet(i)
            u = project(da[1, l, m], pin[l])
            w = project(dc[l, m], pout[l])
            wv_i = lax.dot_general(
                w, dval[l], (((1,), (1,)), ((), ())), precision=EXACT, preferred_element_type=F32
            )
            wv[i] = wv_i
            acc[m] += fold(u * wv_i)
            relay(i)
    loads["ids"].wait()
    loads["prior"].wait()
    domains = prior_mix.shape[0]
    share = domains // n_dp
    mix = prior[...].reshape(1, domains)
    log_mix = jnp.log(mix)
    place = lax.broadcasted_iota(jnp.int32, (1, domains), 1)
    lane = lax.broadcasted_iota(jnp.int32, (1, 128), 1)

    def own(values, j):
        return jnp.sum(jnp.where(place == dp * share + j, values, 0.0), axis=1, keepdims=True)

    early = pl.ds(0, chunks - 1)
    exchange(early, 0).wait_recv()
    sums = []
    for m in range(micro):
        s = acc[m]
        for i in range(m, chunks - 1, micro):
            s += fold(recv[i] * wv[i])
        sums.append(s)
    exchange(chunks - 1, 1).wait_recv()
    sums[micro - 1] += fold(recv[chunks - 1] * wv[chunks - 1])
    mine_row = jnp.zeros((1, 128), F32)
    for m in range(micro):
        s = jnp.sum(jnp.sum(sums[m], axis=0, keepdims=True), axis=1, keepdims=True)
        mine_row += jnp.where(lane == ids[m], s, 0.0)

    row[...] = mine_row
    rows[me] = mine_row

    hops = lambda offset: sum(min(d, n - d) for d, n in zip(offset, (2, ring, ring, ring)))
    offsets = [
        (dc, dx, dy, dz)
        for dc in range(n_e)
        for dx in range(ring)
        for dy in range(ring)
        for dz in range(ring)
    ][1:]
    offsets.sort(key=hops, reverse=True)
    targets = [away(offset) for offset in offsets]
    for k, first in enumerate((n_t, 0)):
        first = jnp.where(me == first, targets[k], first)
        targets[k + 1 :] = [jnp.where(t == first, targets[k], t) for t in targets[k + 1 :]]
        targets[k] = first
    for target in targets:
        pltpu.make_async_remote_copy(
            src_ref=row,
            dst_ref=rows.at[me],
            send_sem=row_send_sem,
            recv_sem=row_recv_sem,
            device_id=target,
            device_id_type=pl.DeviceIdType.LOGICAL,
        ).start()
    everyone = pltpu.make_async_remote_copy(
        src_ref=rows.at[pl.ds(0, devices - 1)],
        dst_ref=rows.at[pl.ds(0, devices - 1)],
        send_sem=row_send_sem,
        recv_sem=row_recv_sem,
        device_id=partner,
        device_id_type=MESH,
    )
    everyone.wait_recv()
    total = jnp.sum(rows.reshape(devices, 128)[...], axis=0, keepdims=True)[:, :domains]
    spread = jnp.sqrt(jnp.sum(total * total, axis=1, keepdims=True) / domains + 1e-06)
    mass = jnp.sum(mix * jnp.exp(0.5 * (total / spread)), axis=1, keepdims=True)
    common = jnp.log(mass)
    answer = jnp.zeros((1, 128), F32)
    for j in range(share):
        picked = own(log_mix, j) + 0.5 * (own(total, j) / spread) - common
        answer = jnp.where(lane == j, picked, answer)
    out[...] = answer[:, :share].reshape(share)

    everyone.wait_send()
    exchange(pl.ds(0, chunks), 0).wait_send()
    for k, helper in enumerate(helpers):

        @pl.when(helper)
        def _():
            pass_on(k).wait_send()
            deliver(k).wait_send()


def per_device(*args):
    (
        dense_act,
        dense_cot,
        dense_proj_in,
        dense_proj_out,
        expert_act,
        expert_cot,
        expert_proj_in,
        expert_proj_out,
        dense_valid,
        expert_valid,
        domain_ids,
        prior_mix,
    ) = args
    sizes = tuple(lax.axis_size(name) for name in ("dp", "expert", "tensor"))
    devices = sizes[0] * sizes[1] * sizes[2]
    layers, micro, tokens, feat = dense_act.shape
    half, width = dense_cot.shape[2:]
    experts, caps, hidden = expert_act.shape[1:]
    slots = expert_cot.shape[2]
    rank = dense_proj_in.shape[2]
    bf = dense_act.dtype
    chunks = micro + layers * micro
    n_loads = 18
    return pl.pallas_call(
        functools.partial(kernel, sizes),
        out_shape=jax.ShapeDtypeStruct((prior_mix.shape[0] // sizes[0],), F32),
        in_specs=[pl.BlockSpec(memory_space=pl.ANY)] * len(args),
        out_specs=pl.BlockSpec(memory_space=pltpu.VMEM),
        scratch_shapes=[
            pltpu.VMEM((2, layers, micro, half, feat), bf),
            pltpu.VMEM((layers, micro, half, width), bf),
            pltpu.VMEM((layers, feat, rank), bf),
            pltpu.VMEM((layers, width, rank), bf),
            pltpu.VMEM((2, micro, experts, slots, hidden), bf),
            pltpu.VMEM((micro, experts, slots, width), bf),
            pltpu.VMEM((hidden, rank), bf),
            pltpu.VMEM((width, rank), bf),
            pltpu.VMEM(dense_valid.shape, F32),
            pltpu.VMEM(expert_valid.shape, F32),
            pltpu.SMEM(domain_ids.shape, jnp.int32),
            pltpu.VMEM(prior_mix.shape, F32),
            pltpu.VMEM((chunks, half, rank), F32),
            pltpu.VMEM((chunks, half, rank), F32),
            pltpu.VMEM((chunks, half, rank), F32),
            pltpu.VMEM((micro, 8, rank), F32),
            pltpu.VMEM((1, 128), F32),
            pltpu.VMEM((devices, 1, 128), F32),
            pltpu.VMEM((len(LIMITS), half // 2, rank), F32),
            pltpu.VMEM((len(LIMITS), half // 2, rank), F32),
            pltpu.SemaphoreType.DMA((4, len(LIMITS))),
            pltpu.SemaphoreType.REGULAR((6,)),
            pltpu.SemaphoreType.DMA((n_loads,)),
            pltpu.SemaphoreType.DMA,
            pltpu.SemaphoreType.DMA((2,)),
            pltpu.SemaphoreType.DMA,
            pltpu.SemaphoreType.DMA,
        ],
        compiler_params=pltpu.CompilerParams(
            collective_id=0, has_side_effects=True, vmem_limit_bytes=56551424
        ),
        name="align",
    )(*args)


def solution(mesh):
    placed = (
        P(None, "dp", "expert", "tensor"),
        P(None, "dp", ("expert", "tensor"), None),
        P(None, "tensor", None),
        P(),
        P("dp", "expert", None, "tensor"),
        P("dp", "expert", "tensor", None),
        P("tensor", None),
        P(),
        P(),
        P("expert", None, None),
        P("dp"),
        P(),
    )
    return jax.shard_map(per_device, mesh=mesh, in_specs=placed, out_specs=P("dp"), check_vma=False)
```

```python
import functools

import jax
import jax.numpy as jnp
from jax import lax
from jax.experimental import pallas as pl
from jax.experimental.pallas import tpu as pltpu
from jax.sharding import PartitionSpec as P

MESH = pl.DeviceIdType.MESH
F32 = jnp.float32
HOLD = 8
KEEP = 5
SPARE = (3, 2)
PASS = 2
DELIVER = (5, 6, 7,)
LIMITS = (21, 24, 28)
EXACT = lax.Precision.HIGHEST


def fold(product):
    rows, lanes = product.shape
    return jnp.sum(product.reshape(rows // 8, 8, lanes), axis=0)


def kernel(
    sizes,
    dense_act,
    dense_cot,
    dense_proj_in,
    dense_proj_out,
    expert_act,
    expert_cot,
    expert_proj_in,
    expert_proj_out,
    dense_valid,
    expert_valid,
    domain_ids,
    prior_mix,
    out,
    da,
    dc,
    pin,
    pout,
    ea,
    ec,
    epin,
    epout,
    dval,
    evalid,
    ids,
    prior,
    send,
    recv,
    wv,
    acc,
    row,
    rows,
    relay_a,
    relay_b,
    relay_sem,
    here,
    load_sem,
    send_sem,
    recv_sem,
    row_send_sem,
    row_recv_sem,
):
    n_dp, n_e, n_t = sizes
    devices = n_dp * n_e * n_t
    dp, ex, te = lax.axis_index("dp"), lax.axis_index("expert"), lax.axis_index("tensor")
    me = (dp * n_e + ex) * n_t + te
    layers, micro = dense_act.shape[0], dense_act.shape[1]
    half = dense_cot.shape[2]
    experts, slots = expert_cot.shape[1], expert_cot.shape[2]
    chunks = micro + layers * micro
    partner = {"tensor": 1 - te}

    ring = 4
    x, y, z = (dp % 2) * 2 + te, (dp // 2) % ring, dp // (2 * ring)

    last = ring - 1

    def number(cc, xx, yy, zz):
        return (((zz * ring + yy) * 2 + xx // n_t) * n_e + cc) * n_t + xx % n_t

    def away(offset):
        dc, dx, dy, dz = offset
        return number((ex + dc) % n_e, (x + dx) % ring, (y + dy) % ring, (z + dz) % ring)

    def signal(semaphore, target):
        pl.semaphore_signal(
            semaphore, inc=1, device_id=target, device_id_type=pl.DeviceIdType.LOGICAL
        )

    def signal_if(condition, semaphore, target):
        @pl.when(condition)
        def _():
            signal(semaphore, target)

    mate, sibling, across = number(ex, x + 1 - 2 * te, y, z), number(1 - ex, x, y, z), number(ex, last - x, y, z)
    mirror = number(ex, last - x, last - y, last - z)
    up_y, down_y = number(ex, x, (y + 1) % ring, z), number(ex, x, (y + last) % ring, z)
    up_z, down_z = number(ex, x, y, (z + 1) % ring), number(ex, x, y, (z + last) % ring)

    def late(xx, yy, zz):
        return 5 * (xx // n_t) + 5 * yy - 4 * (yy // last) + 6 * zz - 4 * (zz // last)

    mine_late, mirror_late = late(x, y, z), late(last - x, last - y, last - z)
    givers = [mine_late >= limit for limit in LIMITS]
    helpers = [mirror_late >= limit for limit in LIMITS]
    helping = helpers[0]

    def hello(k):
        if k == 0:
            semaphore = pltpu.get_barrier_semaphore()
            signal(semaphore, mate)
            signal(semaphore, sibling)
            signal_if(x < n_t, semaphore, across)
            signal_if(helping, semaphore, mirror)
        else:
            semaphore = here.at[k - 1]
        if k == 1:
            signal_if(x >= n_t, semaphore, across)
        if k in (2, 3):
            for target in (mate, sibling, across):
                signal(semaphore, target)
        if k in (0, 2, 3):
            signal_if(y < last, semaphore, up_y)
            signal_if(z < last, semaphore, up_z)
        if k in (1, 2, 3):
            signal_if(y > 0, semaphore, down_y)
            signal_if(z > 0, semaphore, down_z)
        if k in (4, 5):
            for step in range(1, ring):
                signal(semaphore, away((0, step, 0, 0) if k == 4 else (0, 0, step, 0)))
        if k == 6:
            signal(semaphore, sibling)

    from_below = (y + last) // ring + (z + last) // ring
    from_above = 2 - y // last - z // last
    heard = {
        0: 2 + from_below + x // n_t + jnp.where(givers[0], 1, 0),
        1: from_above + 1 - x // n_t,
        2: 3 + from_below + from_above,
        3: 3 + from_below + from_above,
        4: ring - 1,
        5: ring - 1,
        6: 1,
    }

    def listen(k):
        semaphore = pltpu.get_barrier_semaphore() if k == 0 else here.at[k - 1]
        if k == 1:

            @pl.when(heard[k] > 0)
            def _():
                pl.semaphore_wait(semaphore, heard[k])

        else:
            pl.semaphore_wait(semaphore, heard[k])

    other = pl.multiple_of((1 - te) * half, half)
    mine = pl.multiple_of(te * half, half)
    e_other = pl.multiple_of((1 - te) * slots, slots)
    e_mine = pl.multiple_of(te * slots, slots)
    rest = pl.ds(1, micro - 1)
    plan = {
        "epin": (expert_proj_in, epin),
        "first": (expert_act.at[0, 0, pl.ds(e_other, slots), :], ea.at[0, 0, 0]),
        "eao0": (
            expert_act.at[0, pl.ds(1, experts - 1), pl.ds(e_other, slots), :],
            ea.at[0, 0, pl.ds(1, experts - 1)],
        ),
        "eao": (expert_act.at[rest, :, pl.ds(e_other, slots), :], ea.at[0, rest]),
        "pin": (dense_proj_in, pin),
        ("dao", 0): (dense_act.at[0, :, pl.ds(other, half), :], da.at[0, 0]),
        ("dao", 1): (dense_act.at[1, :, pl.ds(other, half), :], da.at[0, 1]),
        "epout": (expert_proj_out, epout),
        "eam": (expert_act.at[:, :, pl.ds(e_mine, slots), :], ea.at[1]),
        "ec": (expert_cot, ec),
        "evalid": (expert_valid, evalid),
        "dval": (dense_valid, dval),
        "ids": (domain_ids, ids),
        "prior": (prior_mix, prior),
        "pout": (dense_proj_out, pout),
        ("dam", 0): (dense_act.at[0, :, pl.ds(mine, half), :], da.at[1, 0]),
        ("dc", 0): (dense_cot.at[0], dc.at[0]),
        ("dam", 1): (dense_act.at[1, :, pl.ds(mine, half), :], da.at[1, 1]),
        ("dc", 1): (dense_cot.at[1], dc.at[1]),
    }
    names = list(plan)
    loads = {
        name: pltpu.make_async_copy(*plan[name], load_sem.at[k]) for k, name in enumerate(names)
    }
    for name in names[:7]:
        loads[name].start()

    hello(0)

    def exchange(part, group):
        return pltpu.make_async_remote_copy(
            src_ref=send.at[part],
            dst_ref=recv.at[part],
            send_sem=send_sem,
            recv_sem=recv_sem.at[group],
            device_id=partner,
            device_id_type=MESH,
        )

    def project(block, weight):
        return jnp.dot(block, weight, preferred_element_type=F32)

    halves = (pl.ds(0, half // 2), pl.ds(half // 2, half // 2))
    units = [(i, part) for i in SPARE for part in halves][: len(LIMITS)]

    def hop(source, target, sent, arrived, device):
        return pltpu.make_async_remote_copy(
            src_ref=source,
            dst_ref=target,
            send_sem=sent,
            recv_sem=arrived,
            device_id=device,
            device_id_type=pl.DeviceIdType.LOGICAL,
        )

    def give(k):
        return hop(send.at[units[k]], relay_a.at[k], send_sem, relay_sem.at[0, k], mirror)

    def pass_on(k):
        return hop(relay_a.at[k], relay_b.at[k], relay_sem.at[1, k], relay_sem.at[2, k], mate)

    def deliver(k):
        return hop(
            relay_b.at[k], recv.at[units[k]], relay_sem.at[3, k], recv_sem.at[0], mirror
        )

    loads["epin"].wait()
    loads["first"].wait()
    head, tail = pl.ds(0, slots), pl.ds(slots, (experts - 1) * slots)
    send[0, head] = project(ea[0, 0, 0], epin[...])
    listen(0)
    exchange((0, head), 0).start()
    for name in names[7:]:
        loads[name].start()
    hello(1)
    loads["eao0"].wait()
    send[0, tail] = project(ea[0, 0, 1:].reshape((experts - 1) * slots, -1), epin[...])
    exchange((0, tail), 0).start()
    loads["eao"].wait()
    for i in SPARE:
        send[i] = project(ea[0, i].reshape(experts * slots, -1), epin[...])
        for part in halves:
            if (i, part) not in units:

                @pl.when(ex == 0)
                def _():
                    exchange((i, part), 0).start()

                continue
            k = units.index((i, part))

            @pl.when(givers[k])
            def _():
                give(k).start()

            direct = jnp.logical_not(givers[k])

            @pl.when(jnp.logical_and(direct, ex == 0) if i != SPARE[0] else direct)
            def _():
                exchange(units[k], 0).start()

    def start(i):
        exchange(i, i // (chunks - 1)).start()

    order = [i for i in range(1, chunks) if i not in SPARE]

    def ready(i):
        if i < KEEP:

            @pl.when(ex == 0)
            def _():
                start(i)

        elif i <= HOLD:

            @pl.when(jnp.logical_and(jnp.logical_not(helping), ex == 0))
            def _():
                start(i)

        else:

            @pl.when(jnp.logical_not(helping))
            def _():
                start(i)

        if i == HOLD:

            @pl.when(ex != 0)
            def _():
                for j in order:
                    if j < KEEP:
                        start(j)

            for j in SPARE[1:]:
                for part in halves:
                    held = ex != 0
                    if (j, part) in units:
                        giving = givers[units.index((j, part))]
                        held = jnp.logical_and(held, jnp.logical_not(giving))

                    @pl.when(held)
                    def _():
                        exchange((j, part), 0).start()

            @pl.when(jnp.logical_and(jnp.logical_not(helping), ex != 0))
            def _():
                for j in order:
                    if KEEP <= j <= HOLD:
                        start(j)

    for m in range(1, micro):
        if m not in SPARE:
            send[m] = project(ea[0, m].reshape(experts * slots, -1), epin[...])
            ready(m)
    loads["pin"].wait()
    for l in range(layers):
        loads["dao", l].wait()
        for m in range(micro):
            i = micro + l * micro + m
            send[i] = project(da[0, l, m], pin[l])
            ready(i)

    meetings = {0: 1, 2: 2, 4: 3, 5: 4, 6: 5, 8: 6}

    def meet(step):
        if step in meetings:
            listen(meetings[step])
            if meetings[step] < 6:
                hello(meetings[step] + 1)

    def relay(step):
        if step == PASS:
            for k, helper in enumerate(helpers):

                @pl.when(helper)
                def _():
                    give(k).wait_recv()
                    pass_on(k).start()

            @pl.when(helping)
            def _():
                for j in order:
                    if j >= KEEP:
                        start(j)

        for k, helper in enumerate(helpers):
            if step == DELIVER[k]:

                @pl.when(helper)
                def _():
                    pass_on(k).wait_recv()
                    deliver(k).start()

    for name in ("epout", "evalid", "dval", "eam", "ec"):
        loads[name].wait()
    for m in range(micro):
        meet(m)
        u = project(ea[1, m].reshape(experts * slots, -1), epin[...])
        w = project(ec[m].reshape(experts * slots, -1), epout[...])
        parts = [
            lax.dot_general(
                w[e * slots : (e + 1) * slots],
                evalid[e],
                (((1,), (1,)), ((), ())),
                precision=EXACT,
                preferred_element_type=F32,
            )
            for e in range(experts)
        ]
        wv_i = jnp.concatenate(parts, axis=0)
        wv[m] = wv_i
        acc[m] = fold(u * wv_i)
        relay(m)
    loads["pout"].wait()
    for l in range(layers):
        loads["dam", l].wait()
        loads["dc", l].wait()
        for m in range(micro):
            i = micro + l * micro + m
            meet(i)
            u = project(da[1, l, m], pin[l])
            w = project(dc[l, m], pout[l])
            wv_i = lax.dot_general(
                w, dval[l], (((1,), (1,)), ((), ())), precision=EXACT, preferred_element_type=F32
            )
            wv[i] = wv_i
            acc[m] += fold(u * wv_i)
            relay(i)
    loads["ids"].wait()
    loads["prior"].wait()
    domains = prior_mix.shape[0]
    share = domains // n_dp
    mix = prior[...].reshape(1, domains)
    log_mix = jnp.log(mix)
    place = lax.broadcasted_iota(jnp.int32, (1, domains), 1)
    lane = lax.broadcasted_iota(jnp.int32, (1, 128), 1)

    def own(values, j):
        return jnp.sum(jnp.where(place == dp * share + j, values, 0.0), axis=1, keepdims=True)

    early = pl.ds(0, chunks - 1)
    exchange(early, 0).wait_recv()
    sums = []
    for m in range(micro):
        s = acc[m]
        for i in range(m, chunks - 1, micro):
            s += fold(recv[i] * wv[i])
        sums.append(s)
    def row_of(m, partial):
        s = jnp.sum(jnp.sum(partial, axis=0, keepdims=True), axis=1, keepdims=True)
        return jnp.where(lane == ids[m], s, 0.0)

    mine_row = row_of(0, sums[0])
    for m in range(1, micro - 1):
        mine_row += row_of(m, sums[m])
    row[...] = mine_row
    exchange(chunks - 1, 1).wait_recv()
    sums[micro - 1] += fold(recv[chunks - 1] * wv[chunks - 1])
    mine_row = row[...] + row_of(micro - 1, sums[micro - 1])

    row[...] = mine_row
    rows[me] = mine_row

    hops = lambda offset: sum(min(d, n - d) for d, n in zip(offset, (2, ring, ring, ring)))
    offsets = [
        (dc, dx, dy, dz)
        for dc in range(n_e)
        for dx in range(ring)
        for dy in range(ring)
        for dz in range(ring)
    ][1:]
    offsets.sort(key=hops, reverse=True)
    targets = [away(offset) for offset in offsets]
    for k, first in enumerate((n_t, 0)):
        first = jnp.where(me == first, targets[k], first)
        targets[k + 1 :] = [jnp.where(t == first, targets[k], t) for t in targets[k + 1 :]]
        targets[k] = first
    for target in targets:
        pltpu.make_async_remote_copy(
            src_ref=row,
            dst_ref=rows.at[me],
            send_sem=row_send_sem,
            recv_sem=row_recv_sem,
            device_id=target,
            device_id_type=pl.DeviceIdType.LOGICAL,
        ).start()
    everyone = pltpu.make_async_remote_copy(
        src_ref=rows.at[pl.ds(0, devices - 1)],
        dst_ref=rows.at[pl.ds(0, devices - 1)],
        send_sem=row_send_sem,
        recv_sem=row_recv_sem,
        device_id=partner,
        device_id_type=MESH,
    )
    everyone.wait_recv()
    total = jnp.sum(rows.reshape(devices, 128)[...], axis=0, keepdims=True)[:, :domains]
    spread = jnp.sqrt(jnp.sum(total * total, axis=1, keepdims=True) / domains + 1e-06)
    mass = jnp.sum(mix * jnp.exp(0.5 * (total / spread)), axis=1, keepdims=True)
    common = jnp.log(mass)
    answer = jnp.zeros((1, 128), F32)
    for j in range(share):
        picked = own(log_mix, j) + 0.5 * (own(total, j) / spread) - common
        answer = jnp.where(lane == j, picked, answer)
    out[...] = answer[:, :share].reshape(share)

    everyone.wait_send()
    exchange(pl.ds(0, chunks), 0).wait_send()
    for k, helper in enumerate(helpers):

        @pl.when(helper)
        def _():
            pass_on(k).wait_send()
            deliver(k).wait_send()


def per_device(*args):
    (
        dense_act,
        dense_cot,
        dense_proj_in,
        dense_proj_out,
        expert_act,
        expert_cot,
        expert_proj_in,
        expert_proj_out,
        dense_valid,
        expert_valid,
        domain_ids,
        prior_mix,
    ) = args
    sizes = tuple(lax.axis_size(name) for name in ("dp", "expert", "tensor"))
    devices = sizes[0] * sizes[1] * sizes[2]
    layers, micro, tokens, feat = dense_act.shape
    half, width = dense_cot.shape[2:]
    experts, caps, hidden = expert_act.shape[1:]
    slots = expert_cot.shape[2]
    rank = dense_proj_in.shape[2]
    bf = dense_act.dtype
    chunks = micro + layers * micro
    n_loads = 19
    return pl.pallas_call(
        functools.partial(kernel, sizes),
        out_shape=jax.ShapeDtypeStruct((prior_mix.shape[0] // sizes[0],), F32),
        in_specs=[pl.BlockSpec(memory_space=pl.ANY)] * len(args),
        out_specs=pl.BlockSpec(memory_space=pltpu.VMEM),
        scratch_shapes=[
            pltpu.VMEM((2, layers, micro, half, feat), bf),
            pltpu.VMEM((layers, micro, half, width), bf),
            pltpu.VMEM((layers, feat, rank), bf),
            pltpu.VMEM((layers, width, rank), bf),
            pltpu.VMEM((2, micro, experts, slots, hidden), bf),
            pltpu.VMEM((micro, experts, slots, width), bf),
            pltpu.VMEM((hidden, rank), bf),
            pltpu.VMEM((width, rank), bf),
            pltpu.VMEM(dense_valid.shape, F32),
            pltpu.VMEM(expert_valid.shape, F32),
            pltpu.SMEM(domain_ids.shape, jnp.int32),
            pltpu.VMEM(prior_mix.shape, F32),
            pltpu.VMEM((chunks, half, rank), F32),
            pltpu.VMEM((chunks, half, rank), F32),
            pltpu.VMEM((chunks, half, rank), F32),
            pltpu.VMEM((micro, 8, rank), F32),
            pltpu.VMEM((1, 128), F32),
            pltpu.VMEM((devices, 1, 128), F32),
            pltpu.VMEM((len(LIMITS), half // 2, rank), F32),
            pltpu.VMEM((len(LIMITS), half // 2, rank), F32),
            pltpu.SemaphoreType.DMA((4, len(LIMITS))),
            pltpu.SemaphoreType.REGULAR((6,)),
            pltpu.SemaphoreType.DMA((n_loads,)),
            pltpu.SemaphoreType.DMA,
            pltpu.SemaphoreType.DMA((2,)),
            pltpu.SemaphoreType.DMA,
            pltpu.SemaphoreType.DMA,
        ],
        compiler_params=pltpu.CompilerParams(
            collective_id=0, has_side_effects=True, vmem_limit_bytes=56551424
        ),
        name="align",
    )(*args)


def solution(mesh):
    placed = (
        P(None, "dp", "expert", "tensor"),
        P(None, "dp", ("expert", "tensor"), None),
        P(None, "tensor", None),
        P(),
        P("dp", "expert", None, "tensor"),
        P("dp", "expert", "tensor", None),
        P("tensor", None),
        P(),
        P(),
        P("expert", None, None),
        P("dp"),
        P(),
    )
    return jax.shard_map(per_device, mesh=mesh, in_specs=placed, out_specs=P("dp"), check_vma=False)
```
